32 devices in a mesh: dp: 4 (over y, x), seq: 8 (over z, core).
Axes of the slice: x: 2, y: 2, z: 4, core: 2. Of those that a mesh axis runs over, the one named last changes fastest.
Arguments:
- tokens: bfloat16 [8, 1024, 2048], P('dp', 'seq'), may hold values from -6 to 6
- cotangent: bfloat16 [8, 1024, 2048], P('dp', 'seq'), may hold values from -6 to 6
- w_query: bfloat16 [2048, 2048], P(('dp', 'seq')), may hold values from -0.1875 to 0.1875
- w_key: bfloat16 [2048, 256], P(('dp', 'seq')), may hold values from -0.1875 to 0.1875
- w_value: bfloat16 [2048, 256], P(('dp', 'seq')), may hold values from -0.125 to 0.125
- w_output: bfloat16 [2048, 2048], P(('dp', 'seq')), may hold values from -0.75 to 0.75
- gain_attn: bfloat16 [2048], P(('dp', 'seq')), may hold values from 0.5 to 1.5
- w_gate: bfloat16 [2048, 5632], P(('dp', 'seq')), may hold values from -0.125 to 0.125
- w_up: bfloat16 [2048, 5632], P(('dp', 'seq')), may hold values from -0.125 to 0.125
- w_down: bfloat16 [5632, 2048], P(('dp', 'seq')), may hold values from -0.109375 to 0.109375
- gain_mlp: bfloat16 [2048], P(('dp', 'seq')), may hold values from 0.5 to 1.5
- span_start: int32 [8, 2], P('dp'), may hold values from 0 to 768, as said below
- span_len: int32 [8, 2], P('dp'), may hold values from 64 to 256
Outputs:
- layer_out: bfloat16 [8, 1024, 2048], P('dp', 'seq')
- input_grad: bfloat16 [8, 1024, 2048], P('dp', 'seq')
- grad_query: float32 [2048, 2048], P(('dp', 'seq'))
- grad_key: float32 [2048, 256], P(('dp', 'seq'))
- grad_value: float32 [2048, 256], P(('dp', 'seq'))
- grad_output: float32 [2048, 2048], P(('dp', 'seq'))
- grad_gain_attn: float32 [2048], P(('dp', 'seq'))
- grad_gate: float32 [2048, 5632], P(('dp', 'seq'))
- grad_up: float32 [2048, 5632], P(('dp', 'seq'))
- grad_down: float32 [5632, 2048], P(('dp', 'seq'))
- grad_gain_mlp: float32 [2048], P(('dp', 'seq'))
The draws below stay inside these ranges and needn't reach their ends.
Inputs may be any that keep to these rules, and one draw needn't show every extreme that they name: `span_start`: the k-th picture of a sequence starts within positions k * 512 to (k + 1) * 512 - 256, so pictures never intersect.
All inputs are finite; a program needn't handle non-finite values.
Results may differ from the reference program's by a relative error of at most 0.02.
Values may be sent and summed in bfloat16 or wider, within the bound.
A program may use at most 384 MiB of HBM per device.

```python
import jax
import jax.numpy as jnp
from jax import lax

D = 2048
H = 32
KVH = 4
HD = 64
FF = 5632
SEQ_LEN = 1024
PIECE = 256
PICS = 2
SEQS = 8


def picture_spans(key):
    region = SEQ_LEN // PICS
    first_key, second_key = jax.random.split(jax.random.fold_in(key, 11))
    lengths = jax.random.randint(first_key, (SEQS, PICS), PIECE // 4, PIECE + 1)
    slot = jnp.arange(PICS, dtype=jnp.int32)[None, :]
    row_index = jnp.arange(SEQS, dtype=jnp.int32)[:, None]
    lengths = jnp.where((row_index == 0) & (slot == 0), PIECE, lengths)
    lengths = jnp.where((row_index == 0) & (slot == 1), PIECE // 4, lengths)
    offsets = jax.random.randint(second_key, (SEQS, PICS), 0, region - PIECE + 1)
    offsets = jnp.where((row_index == 0) & (slot == 0), 0, offsets)
    offsets = jnp.where((row_index == 0) & (slot == PICS - 1), region - PIECE, offsets)
    starts = slot * region + offsets
    return (starts.astype(jnp.int32), lengths.astype(jnp.int32))


def draw_span_start(key, part):
    return picture_spans(key)[0]


def draw_span_len(key, part):
    return picture_spans(key)[1]


def block_levels(stream_key, shape, cuts, least, largest):
    def one(dim, blocks):
        heights = jax.random.uniform(jax.random.fold_in(jax.random.fold_in(stream_key, 6), dim), (blocks,), jnp.float32, least / len(cuts), largest / len(cuts))
        return jnp.repeat(jnp.exp(heights), shape[dim] // blocks).reshape((-1,) + (1,) * (len(shape) - dim - 1))

    level = one(*cuts[0])
    for cut in cuts[1:]:
        level = level * one(*cut)
    return level


def bell_draw(key, dims, spread, bound, cuts=(), held_as=jnp.bfloat16):
    drawn = jax.random.normal(key, dims, jnp.float32) * spread
    if len(cuts) > 0:
        drawn = block_levels(key, dims, cuts, -0.22, 0.18) * drawn
    return jnp.clip(drawn, min=-bound, max=bound).astype(held_as)


def setup_inputs(seed: int = 0) -> dict:
    streams_of = jax.random.split(jax.random.key(seed), 14)
    tokens = bell_draw(streams_of[0], (SEQS, SEQ_LEN, D), 1.0, 6.0, ((0, 4), (1, 8)))
    cotangent = bell_draw(streams_of[1], (SEQS, SEQ_LEN, D), 1.0, 6.0, ((0, 4), (1, 8)))
    w_query = bell_draw(streams_of[2], (D, D), (D // 2) ** -0.5, 0.1875, ((0, 32),))
    w_key = bell_draw(streams_of[3], (D, KVH * HD), (D // 2) ** -0.5, 0.1875, ((0, 32),))
    w_value = bell_draw(streams_of[4], (D, KVH * HD), D ** -0.5, 0.125, ((0, 32),))
    w_output = bell_draw(streams_of[5], (D, D), (D // 32) ** -0.5, 0.75, ((0, 32),))
    gain_attn = jnp.clip(1.0 + 0.1 * jax.random.normal(streams_of[6], (D,), jnp.float32), 0.5, 1.5).astype(jnp.bfloat16)
    w_gate = bell_draw(streams_of[7], (D, FF), D ** -0.5, 0.125, ((0, 32),))
    w_up = bell_draw(streams_of[8], (D, FF), D ** -0.5, 0.125, ((0, 32),))
    w_down = bell_draw(streams_of[9], (FF, D), (FF // 2) ** -0.5, 0.109375, ((0, 32),))
    gain_mlp = jnp.clip(1.0 + 0.1 * jax.random.normal(streams_of[10], (D,), jnp.float32), 0.5, 1.5).astype(jnp.bfloat16)
    span_start = draw_span_start(jax.random.fold_in(streams_of[13], 71), 0)
    span_len = draw_span_len(jax.random.fold_in(streams_of[13], 71), 0)
    return {"tokens": tokens, "cotangent": cotangent, "w_query": w_query, "w_key": w_key, "w_value": w_value, "w_output": w_output, "gain_attn": gain_attn, "w_gate": w_gate, "w_up": w_up, "w_down": w_down, "gain_mlp": gain_mlp, "span_start": span_start, "span_len": span_len}


epsilon = 1e-05
masked_value = -1e+30
rope_base = 10000.0

@jax.custom_vjp
def low(v):
    return lax.optimization_barrier(v.astype(jnp.bfloat16)).astype(jnp.float32)

@jax.custom_vjp
def low_back(v):
    return v

def low_keep(v):
    return (low(v), None)

def low_pass(kept, grad):
    return (grad,)

def back_keep(v):
    return (v, None)

def back_low(kept, grad):
    return (low(grad),)
low.defvjp(low_keep, low_pass)
low_back.defvjp(back_keep, back_low)

def rope_tables(positions, half_width):
    frequency = rope_base ** (-jnp.arange(half_width, dtype=jnp.float32) / half_width)
    angles = positions.astype(jnp.float32)[:, None] * frequency[None, :]
    return (jnp.cos(angles), jnp.sin(angles))

def rotate(values, cosine, sine):
    half_width = values.shape[-1] // 2
    first_half = values[..., :half_width]
    second_half = values[..., half_width:]
    cosine_rows = cosine[:, None, :]
    sine_rows = sine[:, None, :]
    return jnp.concatenate([first_half * cosine_rows - second_half * sine_rows, second_half * cosine_rows + first_half * sine_rows], axis=-1)

def picture_of(positions, starts, lengths):
    inside = (positions[..., None, :] >= starts[..., :, None]) & (positions[..., None, :] < (starts + lengths)[..., :, None])
    labels = jnp.arange(1, starts.shape[-1] + 1, dtype=jnp.int32)
    return (lax.optimization_barrier(jnp.sum(jnp.where(inside, labels[:, None], 0), axis=-2)) - 1).astype(jnp.int32)

def rms_scale(values):
    return lax.rsqrt(lax.optimization_barrier(jnp.mean(values * values, axis=-1, keepdims=True)) + epsilon)

def attention(queries, key_rows, value_rows, positions, pictures):
    length_total = queries.shape[0]
    block_rows = min(512, length_total)
    block_count = length_total // block_rows
    score_scale = 1.0 / HD ** 0.5
    highest = lax.Precision.HIGHEST

    def one_block(block_item):
        query_block, query_pos, query_pic = block_item
        scores = jnp.einsum('qcgd,kcd->cgqk', query_block, key_rows, precision=highest) * score_scale
        scores = low_back(scores)
        allowed = (positions[None, :] <= query_pos[:, None]) | (query_pic[:, None] == pictures[None, :]) & (query_pic[:, None] >= 0)
        scores = jnp.where(allowed[None, None], scores, masked_value)
        row_top = lax.optimization_barrier(jnp.max(scores, axis=-1, keepdims=True))
        exponent = jnp.exp(scores - row_top)
        probability = exponent / lax.optimization_barrier(jnp.sum(exponent, axis=-1, keepdims=True))
        mixture = jnp.einsum('cgqk,kcd->qcgd', low(probability), value_rows, precision=highest)
        return low(low_back(mixture)).reshape(block_rows, -1)
    pieces = lax.map(jax.checkpoint(one_block), (queries.reshape((block_count, block_rows) + queries.shape[1:]), positions.reshape(block_count, block_rows), pictures.reshape(block_count, block_rows)))
    return pieces.reshape(length_total, -1)

def layer(inputs, w_query, w_key, w_value, w_output, gain_attn, w_gate, w_up, w_down, gain_mlp, positions, pictures, cosine, sine):
    length_total = inputs.shape[0]
    highest = lax.Precision.HIGHEST
    normed = low(inputs * rms_scale(inputs) * gain_attn)
    query_pre = low_back(jnp.dot(normed, w_query, precision=highest, preferred_element_type=jnp.float32))
    key_pre = low_back(jnp.dot(normed, w_key, precision=highest, preferred_element_type=jnp.float32))
    value_pre = low_back(jnp.dot(normed, w_value, precision=highest, preferred_element_type=jnp.float32))
    queries = low(rotate(query_pre.reshape(length_total, H, HD), cosine, sine)).reshape(length_total, KVH, H // KVH, HD)
    key_rows = low(rotate(key_pre.reshape(length_total, KVH, HD), cosine, sine))
    value_rows = low(value_pre).reshape(length_total, KVH, HD)
    attended = attention(queries, key_rows, value_rows, positions, pictures)
    middle = inputs + low_back(jnp.dot(attended, w_output, precision=highest, preferred_element_type=jnp.float32))
    normed_mid = low(middle * rms_scale(middle) * gain_mlp)
    gate_pre = low_back(jnp.dot(normed_mid, w_gate, precision=highest, preferred_element_type=jnp.float32))
    up_pre = low_back(jnp.dot(normed_mid, w_up, precision=highest, preferred_element_type=jnp.float32))
    hidden = low(low_back(gate_pre * jax.nn.sigmoid(gate_pre) * up_pre))
    return middle + jnp.dot(hidden, w_down, precision=highest, preferred_element_type=jnp.float32)

def reference(tokens, cotangent, w_query, w_key, w_value, w_output, gain_attn, w_gate, w_up, w_down, gain_mlp, span_start, span_len):
    weights = tuple((weight_item.astype(jnp.float32) for weight_item in (w_query, w_key, w_value, w_output, gain_attn, w_gate, w_up, w_down, gain_mlp)))
    positions = jnp.arange(SEQ_LEN, dtype=jnp.int32)
    cosine, sine = rope_tables(positions, HD // 2)

    def one_sequence(totals, sequence_item):
        seq_tokens, seq_grad, seq_starts, seq_lengths = sequence_item
        pictures = picture_of(positions, seq_starts, seq_lengths)

        def forward(inputs, *params):
            return layer(inputs, *params, positions, pictures, cosine, sine)
        outputs, pullback = jax.vjp(forward, seq_tokens.astype(jnp.float32), *weights)
        gradients = pullback(seq_grad.astype(jnp.float32))
        new_totals = tuple((running + extra for running, extra in zip(totals, gradients[1:])))
        return (new_totals, (outputs.astype(jnp.bfloat16), gradients[0].astype(jnp.bfloat16)))
    initial = tuple((jnp.zeros_like(weight_item) for weight_item in weights))
    totals, (layer_out, input_grad) = lax.scan(one_sequence, initial, (tokens, cotangent, span_start, span_len))
    return (layer_out, input_grad, totals[0], totals[1], totals[2], totals[3], totals[4], totals[5], totals[6], totals[7], totals[8])
```

```python
import functools
import math

import jax
import jax.numpy as jnp
from jax import lax
from jax.experimental import pallas as pl
from jax.experimental.pallas import tpu as pltpu
from jax.sharding import Mesh, PartitionSpec as P

H = 32
KVH = 4
HD = 64
HALF = HD // 2

epsilon = 1e-05
masked_value = -1e30
rope_base = 10000.0

PLANE = ("dp", "core")
ALL = ("dp", "zz", "core")
f32 = jnp.float32
bf16 = jnp.bfloat16


def rms_scale(values):
    return lax.rsqrt(jnp.mean(values * values, axis=-1, keepdims=True) + epsilon)


def rms_back(grad_normed, values, inverse, gain):
    scaled_grad = grad_normed * gain
    unit_rows = values * inverse
    grad_values = inverse * (
        scaled_grad - unit_rows * jnp.mean(scaled_grad * unit_rows, axis=-1, keepdims=True)
    )
    return (grad_values, jnp.sum(grad_normed * unit_rows, axis=0))


def swap_halves(values):
    width = values.shape[-1]
    lane = lax.broadcasted_iota(jnp.int32, values.shape, 1)
    ahead = pltpu.roll(values, width - HALF, 1)
    behind = pltpu.roll(values, HALF, 1)
    return jnp.where(lane % HD < HALF, -ahead, behind)


def span_bias(scalars, seq_index, pics, seqs, keys, queries):
    key_pos = lax.broadcasted_iota(jnp.int32, (keys, 1), 0)
    query_pos = lax.broadcasted_iota(jnp.int32, (1, queries), 1) + scalars[2 * seqs * pics]
    allowed = key_pos <= query_pos
    for k in range(pics):
        start = scalars[seq_index * pics + k]
        stop = start + scalars[seqs * pics + seq_index * pics + k]
        key_in = (key_pos >= start) & (key_pos < stop)
        query_in = (query_pos >= start) & (query_pos < stop)
        allowed = allowed | (key_in & query_in)
    return jnp.where(allowed, 0.0, masked_value).astype(f32)


def rows_dot(left, right):
    return lax.dot_general(left, right, (((1,), (1,)), ((), ())), preferred_element_type=f32)


def attend_kernel(pics, seqs, heads, scalars, pre_ref, cos_ref, sin_ref, kv_ref, out_ref, q_ref, lse_ref):
    seq_index = pl.program_id(0)
    cores, rows = pre_ref.shape[1], pre_ref.shape[3]
    queries, keys = cores * rows, kv_ref.shape[1]
    width = heads * HD
    pre = pre_ref[0, :, 0, :, :width].reshape(queries, width)
    q = (pre * cos_ref[...] + swap_halves(pre) * sin_ref[...]).astype(bf16) * bf16(0.125)
    q_ref[...] = q.reshape(q_ref.shape)
    kv = kv_ref[0]
    k = kv[:, :HD]
    v_t = kv.T[HD:]
    bias = span_bias(scalars, seq_index, pics, seqs, keys, queries)
    outs = []
    for h in range(heads):
        s = rows_dot(k, q[:, h * HD : (h + 1) * HD]) + bias
        top = jnp.max(s, axis=0, keepdims=True)
        e = jnp.exp(s - top)
        total = jnp.sum(e, axis=0, keepdims=True)
        p = (e * (1.0 / total)).astype(bf16)
        lse_ref[0, h : h + 1, :] = top + jnp.log(total)
        outs.append(jnp.dot(v_t, p, preferred_element_type=f32))
    out = jnp.concatenate(outs, axis=0).T.astype(bf16)
    out_ref[...] = out.reshape(out_ref.shape)


def attend_back_kernel(
    pics, seqs, heads, scalars, q_ref, do_ref, cos_ref, sin_ref, kv_ref, lse_ref, dq_ref, dkv_ref
):
    seq_index = pl.program_id(0)
    cores, rows = q_ref.shape[1], q_ref.shape[3]
    queries, keys = cores * rows, kv_ref.shape[1]
    width = heads * HD
    q = q_ref[...].reshape(queries, width)
    do = do_ref[...].reshape(queries, width)
    kv = kv_ref[0]
    k, v = kv[:, :HD], kv[:, HD:]
    k_t = kv.T[:HD]
    bias = span_bias(scalars, seq_index, pics, seqs, keys, queries)
    dk = jnp.zeros((keys, HD), f32)
    dv = jnp.zeros((keys, HD), f32)
    dqs = []
    for h in range(heads):
        q_h = q[:, h * HD : (h + 1) * HD]
        do_h = do[:, h * HD : (h + 1) * HD]
        p = jnp.exp(rows_dot(k, q_h) + bias - lse_ref[0, h : h + 1, :])
        dp = rows_dot(v, do_h)
        delta = jnp.sum(p * dp, axis=0, keepdims=True)
        ds = (p * (dp - delta)).astype(bf16)
        dv = dv + jnp.dot(p.astype(bf16), do_h, preferred_element_type=f32)
        dk = dk + jnp.dot(ds, q_h, preferred_element_type=f32)
        dqs.append(jnp.dot(k_t, ds, preferred_element_type=f32))
    dq = jnp.concatenate(dqs, axis=0).T * 0.125
    dqp = dq * cos_ref[...] - swap_halves(dq) * sin_ref[...]
    dq_ref[...] = dqp.astype(bf16).reshape(dq_ref.shape)
    dkv_ref[0] = jnp.concatenate([dk, dv], axis=1).astype(bf16)


def plane_gather(values):
    return lax.all_gather(values, PLANE, axis=0, tiled=True)


def plane_reduce(values):
    return lax.psum_scatter(values, PLANE, scatter_dimension=0, tiled=True)


def local(
    tokens,
    cotangent,
    w_query,
    w_key,
    w_value,
    w_output,
    gain_attn,
    w_gate,
    w_up,
    w_down,
    gain_mlp,
    span_start,
    span_len,
):
    nd, nz, nc = lax.axis_size("dp"), lax.axis_size("zz"), lax.axis_size("core")
    plane = nd * nc
    seq_count, row_count, width = tokens.shape
    own = seq_count * row_count
    group = plane * own
    held = w_query.shape[0]
    ff_held = w_down.shape[0]
    heads = H // plane
    q_width = heads * HD
    seqs = nd * seq_count
    pics = span_start.shape[1]
    queries = nc * row_count
    zz, core = lax.axis_index("zz"), lax.axis_index("core")
    whole_heads = held % HD == 0

    def to_inner(values):
        shape = values.shape
        values = values.reshape(shape[:-1] + (nd, nz, nc * held))
        return values.swapaxes(-3, -2).reshape(shape)

    def to_outer(values):
        shape = values.shape
        values = values.reshape(shape[:-1] + (nz, nd, nc * held))
        return values.swapaxes(-3, -2).reshape(shape)

    def by_member(weight, unit):
        weight = weight.reshape(held, nd, nz, nc, unit)
        return weight.transpose(1, 3, 0, 2, 4).reshape(plane, held, nz * unit)

    def from_member(parts, unit):
        parts = parts.reshape(nd, nc, held, nz, unit)
        return parts.transpose(2, 0, 3, 1, 4).reshape(held, nd * nz * nc * unit)

    if whole_heads:
        query_cols = by_member(w_query, held)
    else:
        query_cols = w_query.reshape(held, plane, q_width).transpose(1, 0, 2)
    share = plane // KVH
    key_cols = jnp.repeat(w_key.reshape(held, KVH, HD).transpose(1, 0, 2), share, axis=0)
    value_cols = jnp.repeat(w_value.reshape(held, KVH, HD).transpose(1, 0, 2), share, axis=0)
    columns = jnp.concatenate(
        [query_cols, key_cols, value_cols, by_member(w_gate, ff_held), by_member(w_up, ff_held)],
        axis=-1,
    )
    columns = lax.all_to_all(columns, PLANE, 0, 0, tiled=True)
    qkv_width = q_width + 2 * HD
    ff_width = nz * ff_held

    def z_gather(values):
        return lax.all_gather(values, "zz", axis=0, tiled=True)

    gains = lax.all_gather(jnp.stack([gain_attn, gain_mlp]), ALL, axis=1, tiled=True).astype(f32)
    gain_a, gain_m = gains[0], gains[1]
    spans = lax.all_gather(
        jnp.concatenate([span_start, span_len], axis=1), "dp", axis=0, tiled=True
    )
    scalars = jnp.concatenate(
        [
            spans[:, :pics].reshape(-1),
            spans[:, pics:].reshape(-1),
            (zz * queries).astype(jnp.int32)[None],
        ]
    )

    wqkv = z_gather(columns[:, :, :qkv_width].reshape(plane * held, qkv_width))
    if whole_heads:
        wo = z_gather(w_output)
    else:
        wo = lax.all_gather(w_output, ("zz", "core"), axis=0, tiled=True)
        wo = lax.dynamic_slice_in_dim(wo, core * q_width, q_width, 0)
    wg = z_gather(columns[:, :, qkv_width : qkv_width + ff_width].reshape(plane * held, ff_width))
    wu = z_gather(columns[:, :, qkv_width + ff_width :].reshape(plane * held, ff_width))
    wd = z_gather(w_down)

    positions = (zz * queries + jnp.arange(queries, dtype=jnp.int32)).astype(f32)
    frequency = rope_base ** (-jnp.arange(HALF, dtype=f32) / HALF)
    angles = positions[:, None] * frequency[None, :]
    cosine, sine = jnp.cos(angles), jnp.sin(angles)
    cos_wide = jnp.tile(cosine, (1, q_width // HALF))
    sin_wide = jnp.tile(sine, (1, q_width // HALF))
    cos_k = cosine.reshape(1, nc, 1, row_count, HALF)
    sin_k = sine.reshape(1, nc, 1, row_count, HALF)

    x_low = tokens.reshape(own, width)
    x = x_low.astype(f32)
    inverse_attn = rms_scale(x)
    x_group = plane_gather(x_low).astype(f32)
    normed = to_inner((x_group * rms_scale(x_group) * gain_a).astype(bf16))
    dy_low = cotangent.reshape(own, width)
    dy_group = plane_gather(dy_low)

    pre = jnp.dot(normed, wqkv, preferred_element_type=f32)
    pre = pre.reshape(nd, nc, seq_count, row_count, qkv_width)
    ka, kb = pre[..., q_width : q_width + HALF], pre[..., q_width + HALF : q_width + HD]
    kv = jnp.concatenate(
        [ka * cos_k - kb * sin_k, kb * cos_k + ka * sin_k, pre[..., q_width + HD :]], axis=-1
    ).astype(bf16)
    kv = kv.transpose(0, 2, 1, 3, 4).reshape(seqs, queries, 2 * HD)
    kv_all = lax.all_gather(kv, "zz", axis=1, tiled=True)
    keys = nz * queries

    def token_block(columns_held):
        return pl.BlockSpec(
            (1, nc, 1, row_count, columns_held),
            lambda g, s: (g // seq_count, 0, lax.rem(g, seq_count), 0, 0),
        )

    table_block = pl.BlockSpec((queries, q_width), lambda g, s: (0, 0))
    kv_block = pl.BlockSpec((1, keys, 2 * HD), lambda g, s: (g, 0, 0))
    lse_block = pl.BlockSpec((1, heads, queries), lambda g, s: (g, 0, 0))
    token_shape = jax.ShapeDtypeStruct((nd, nc, seq_count, row_count, q_width), bf16)

    attended, q_kept, lse = pl.pallas_call(
        functools.partial(attend_kernel, pics, seqs, heads),
        out_shape=(
            token_shape,
            token_shape,
            jax.ShapeDtypeStruct((seqs, heads, queries), f32),
        ),
        grid_spec=pltpu.PrefetchScalarGridSpec(
            num_scalar_prefetch=1,
            grid=(seqs,),
            in_specs=[token_block(qkv_width), table_block, table_block, kv_block],
            out_specs=(token_block(q_width), token_block(q_width), lse_block),
        ),
        cost_estimate=pl.CostEstimate(
            flops=4 * seqs * heads * queries * keys * HD,
            bytes_accessed=8 * group * q_width,
            transcendentals=seqs * heads * queries * keys,
        ),
    )(scalars, pre, cos_wide, sin_wide, kv_all)

    attended = attended.reshape(group, q_width)
    mixed = plane_reduce(jnp.dot(attended, wo, preferred_element_type=f32).astype(bf16))
    middle = x + mixed.astype(f32)
    inverse_mlp = rms_scale(middle)
    normed_mid = plane_gather(to_inner((middle * inverse_mlp * gain_m).astype(bf16)))
    gate = jnp.dot(normed_mid, wg, preferred_element_type=f32)
    up = jnp.dot(normed_mid, wu, preferred_element_type=f32)
    sigmoid = jax.nn.sigmoid(gate)
    hidden = (gate * sigmoid * up).astype(bf16)
    grad_hidden = rows_dot(dy_group, wd).astype(bf16).astype(f32)
    grad_gate = (grad_hidden * up * sigmoid * (1.0 + gate * (1.0 - sigmoid))).astype(bf16)
    grad_up = (grad_hidden * gate * sigmoid).astype(bf16)

    back_mid = plane_reduce((rows_dot(grad_gate, wg) + rows_dot(grad_up, wu)).astype(bf16))
    grad_normed_mid = to_outer(back_mid.astype(f32))
    grad_middle_norm, part_gain_mlp = rms_back(grad_normed_mid, middle, inverse_mlp, gain_m)
    grad_middle = dy_low.astype(f32) + grad_middle_norm
    mid_group = plane_gather(grad_middle.astype(bf16))
    grad_mix = rows_dot(mid_group, wo).astype(bf16)

    down = plane_reduce(jnp.dot(hidden, wd, preferred_element_type=f32).astype(bf16))
    layer_out = (middle + down.astype(f32)).astype(bf16).reshape(tokens.shape)

    dq, dkv = pl.pallas_call(
        functools.partial(attend_back_kernel, pics, seqs, heads),
        out_shape=(token_shape, jax.ShapeDtypeStruct((seqs, keys, 2 * HD), bf16)),
        grid_spec=pltpu.PrefetchScalarGridSpec(
            num_scalar_prefetch=1,
            grid=(seqs,),
            in_specs=[
                token_block(q_width),
                token_block(q_width),
                table_block,
                table_block,
                kv_block,
                lse_block,
            ],
            out_specs=(token_block(q_width), kv_block),
        ),
        cost_estimate=pl.CostEstimate(
            flops=10 * seqs * heads * queries * keys * HD,
            bytes_accessed=8 * group * q_width,
            transcendentals=seqs * heads * queries * keys,
        ),
    )(
        scalars,
        q_kept,
        grad_mix.reshape(token_shape.shape),
        cos_wide,
        sin_wide,
        kv_all,
        lse,
    )
    dkv = lax.psum_scatter(dkv, "zz", scatter_dimension=1, tiled=True).astype(f32)
    dkv = dkv.reshape(nd, seq_count, nc, row_count, 2 * HD).transpose(0, 2, 1, 3, 4)
    da, db = dkv[..., :HALF], dkv[..., HALF:HD]
    dkv = jnp.concatenate(
        [da * cos_k + db * sin_k, db * cos_k - da * sin_k, dkv[..., HD:]], axis=-1
    ).astype(bf16)
    dqkv = jnp.concatenate(
        [dq.reshape(group, q_width), dkv.reshape(group, 2 * HD)], axis=-1
    )
    back_in = plane_reduce(rows_dot(dqkv, wqkv).astype(bf16))
    grad_normed = to_outer(back_in.astype(f32))
    grad_input_norm, part_gain_attn = rms_back(grad_normed, x, inverse_attn, gain_a)
    input_grad = (grad_middle + grad_input_norm).astype(bf16).reshape(tokens.shape)

    def columns_dot(left, right):
        return lax.dot_general(
            left, right, (((0,), (0,)), ((), ())), preferred_element_type=f32
        ).astype(bf16)

    def z_reduce(values):
        return lax.psum_scatter(values, "zz", scatter_dimension=0, tiled=True)

    def home(values):
        values = values.reshape(plane, held, values.shape[-1])
        return lax.all_to_all(values, PLANE, 0, 0, tiled=True).astype(f32)

    weight_down = z_reduce(columns_dot(hidden, dy_group)).astype(f32)
    weight_gate = from_member(home(z_reduce(columns_dot(normed_mid, grad_gate))), ff_held)
    weight_up = from_member(home(z_reduce(columns_dot(normed_mid, grad_up))), ff_held)
    weight_output = columns_dot(attended, mid_group)
    if whole_heads:
        weight_output = z_reduce(weight_output).astype(f32)
    else:
        spread = lax.dynamic_update_slice_in_dim(
            jnp.zeros((nc * q_width, width), bf16), weight_output, core * q_width, 0
        )
        weight_output = lax.psum_scatter(
            spread, ("zz", "core"), scatter_dimension=0, tiled=True
        ).astype(f32)
    weight_qkv = home(z_reduce(columns_dot(normed, dqkv)))
    if whole_heads:
        weight_query = from_member(weight_qkv[:, :, :q_width], held)
    else:
        weight_query = weight_qkv[:, :, :q_width].transpose(1, 0, 2).reshape(held, H * HD)

    def kv_home(parts):
        parts = jnp.sum(parts.reshape(KVH, share, held, HD), axis=1)
        return parts.transpose(1, 0, 2).reshape(held, KVH * HD)

    weight_key = kv_home(weight_qkv[:, :, q_width : q_width + HD])
    weight_value = kv_home(weight_qkv[:, :, q_width + HD :])
    gain_grads = lax.psum_scatter(
        jnp.stack([part_gain_attn, part_gain_mlp]), ALL, scatter_dimension=1, tiled=True
    )
    return (
        layer_out,
        input_grad,
        weight_query,
        weight_key,
        weight_value,
        weight_output,
        gain_grads[0],
        weight_gate,
        weight_up,
        weight_down,
        gain_grads[1],
    )


def solution(mesh):
    nd, ns = mesh.shape["dp"], mesh.shape["seq"]
    inner = Mesh(mesh.devices.reshape(nd, ns // 2, 2), ALL)
    rows = P("dp", ("zz", "core"), None)
    weight = P(ALL, None)
    gain = P(ALL)
    spans = P("dp", None)
    return jax.shard_map(
        local,
        mesh=inner,
        in_specs=(rows, rows) + (weight,) * 4 + (gain,) + (weight,) * 3 + (gain, spans, spans),
        out_specs=(rows, rows) + (weight,) * 4 + (gain,) + (weight,) * 3 + (gain,),
        check_vma=False,
    )
```

```python
import functools

import jax
import jax.numpy as jnp
from jax import lax
from jax.experimental import pallas as pl
from jax.experimental.pallas import tpu as pltpu
from jax.sharding import Mesh, PartitionSpec as P


H = 32
KVH = 4
HD = 64
HALF = HD // 2

epsilon = 1e-05
masked_value = -1e30
rope_base = 10000.0

PLANE = ("dp", "core")
ALL = ("dp", "zz", "core")
f32 = jnp.float32
bf16 = jnp.bfloat16


def rms_scale(values):
    return lax.rsqrt(jnp.mean(values * values, axis=-1, keepdims=True) + epsilon)


def rms_back(grad_normed, values, inverse, gain):
    scaled_grad = grad_normed * gain
    unit_rows = values * inverse
    grad_values = inverse * (
        scaled_grad - unit_rows * jnp.mean(scaled_grad * unit_rows, axis=-1, keepdims=True)
    )
    return grad_values


def swap_halves(values):
    width = values.shape[-1]
    lane = lax.broadcasted_iota(jnp.int32, values.shape, 1)
    ahead = pltpu.roll(values, width - HALF, 1)
    behind = pltpu.roll(values, HALF, 1)
    return jnp.where(lane % HD < HALF, -ahead, behind)


def span_bias(scalars, seq_index, pics, seqs, keys, queries):
    key_pos = lax.broadcasted_iota(jnp.int32, (keys, 1), 0)
    query_pos = lax.broadcasted_iota(jnp.int32, (1, queries), 1) + scalars[2 * seqs * pics]
    allowed = key_pos <= query_pos
    for k in range(pics):
        start = scalars[seq_index * pics + k]
        stop = start + scalars[seqs * pics + seq_index * pics + k]
        key_in = (key_pos >= start) & (key_pos < stop)
        query_in = (query_pos >= start) & (query_pos < stop)
        allowed = allowed | (key_in & query_in)
    return jnp.where(allowed, 0.0, masked_value).astype(f32)


def rows_dot(left, right):
    return lax.dot_general(left, right, (((1,), (1,)), ((), ())), preferred_element_type=f32)


def attend_kernel(pics, seqs, heads, scalars, pre_ref, cos_ref, sin_ref, kv_ref, out_ref, q_ref, lse_ref):
    seq_index = pl.program_id(0)
    cores, rows = pre_ref.shape[1], pre_ref.shape[3]
    queries, keys = cores * rows, kv_ref.shape[1]
    width = heads * HD
    pre = pre_ref[0, :, 0, :, :width].reshape(queries, width)
    q = (pre * cos_ref[...] + swap_halves(pre) * sin_ref[...]).astype(bf16) * bf16(0.125)
    q_ref[...] = q.reshape(q_ref.shape)
    kv = kv_ref[0]
    k = kv[:, :HD]
    v_t = kv.T[HD:]
    bias = span_bias(scalars, seq_index, pics, seqs, keys, queries)
    outs = []
    for h in range(heads):
        s = rows_dot(k, q[:, h * HD : (h + 1) * HD]) + bias
        top = jnp.max(s, axis=0, keepdims=True)
        e = jnp.exp(s - top)
        total = jnp.sum(e, axis=0, keepdims=True)
        p = (e * (1.0 / total)).astype(bf16)
        lse_ref[0, h : h + 1, :] = top + jnp.log(total)
        outs.append(jnp.dot(v_t, p, preferred_element_type=f32))
    out = jnp.concatenate(outs, axis=0).T.astype(bf16)
    out_ref[...] = out.reshape(out_ref.shape)


def attend_back_kernel(
    pics, seqs, heads, scalars, q_ref, do_ref, cos_ref, sin_ref, kv_ref, lse_ref, dq_ref, dkv_ref
):
    seq_index = pl.program_id(0)
    cores, rows = q_ref.shape[1], q_ref.shape[3]
    queries, keys = cores * rows, kv_ref.shape[1]
    width = heads * HD
    q = q_ref[...].reshape(queries, width)
    do = do_ref[...].reshape(queries, width)
    kv = kv_ref[0]
    k, v = kv[:, :HD], kv[:, HD:]
    k_t = kv.T[:HD]
    bias = span_bias(scalars, seq_index, pics, seqs, keys, queries)
    dk = jnp.zeros((keys, HD), f32)
    dv = jnp.zeros((keys, HD), f32)
    dqs = []
    for h in range(heads):
        q_h = q[:, h * HD : (h + 1) * HD]
        do_h = do[:, h * HD : (h + 1) * HD]
        p = jnp.exp(rows_dot(k, q_h) + bias - lse_ref[0, h : h + 1, :])
        dp = rows_dot(v, do_h)
        delta = jnp.sum(p * dp, axis=0, keepdims=True)
        ds = (p * (dp - delta)).astype(bf16)
        dv = dv + jnp.dot(p.astype(bf16), do_h, preferred_element_type=f32)
        dk = dk + jnp.dot(ds, q_h, preferred_element_type=f32)
        dqs.append(jnp.dot(k_t, ds, preferred_element_type=f32))
    dq = jnp.concatenate(dqs, axis=0).T * 0.125
    dqp = dq * cos_ref[...] - swap_halves(dq) * sin_ref[...]
    dq_ref[...] = dqp.astype(bf16).reshape(dq_ref.shape)
    dkv_ref[0] = jnp.concatenate([dk, dv], axis=1).astype(bf16)


MESH = pl.DeviceIdType.MESH
PARTS = 2
CHUNKS = 2


def flip(index, mask):
    bit = 1
    while bit <= mask:
        if mask & bit:
            index = index + bit - 2 * bit * (index // bit % 2)
        bit *= 2
    return index


def hops(nd):
    bits = [1 << i for i in range(nd.bit_length() - 1)]
    return (bits, bits[::-1])


def greet(nd, dp, other):
    barrier = pltpu.get_barrier_semaphore()
    bits = hops(nd)[0]
    for bit in bits:
        pl.semaphore_signal(
            barrier, inc=1, device_id={"dp": flip(dp, bit)}, device_id_type=MESH
        )
    pl.semaphore_signal(barrier, inc=1, device_id={"core": other}, device_id_type=MESH)
    pl.semaphore_wait(barrier, len(bits) + 1)


def spread_kernel(nd, x_ref, out_ref, held, keep_sem, send, recv, core_send, core_recv):
    dp, core = lax.axis_index("dp"), lax.axis_index("core")
    other = 1 - core
    rows = x_ref.shape[0] // (PARTS * CHUNKS)
    greet(nd, dp, other)
    orders = hops(nd)
    pieces = [(c, p) for c in range(CHUNKS) for p in range(PARTS)]

    def span(c, p):
        return pl.ds((p * CHUNKS + c) * rows, rows)

    def hop(c, p, mask, bit):
        place = out_ref.at[flip(dp, mask), core, span(c, p)]
        source = x_ref.at[span(c, p)] if mask == 0 else place
        index = (p * CHUNKS + c) * nd + mask + bit
        return pltpu.make_async_remote_copy(
            src_ref=source,
            dst_ref=place,
            send_sem=send.at[index],
            recv_sem=recv.at[index],
            device_id={"dp": flip(dp, bit)},
            device_id_type=MESH,
        )

    def share(c, p, mask):
        place = out_ref.at[flip(dp, mask), core, span(c, p)]
        source = x_ref.at[span(c, p)] if mask == 0 else place
        index = (p * CHUNKS + c) * nd + mask
        return pltpu.make_async_remote_copy(
            src_ref=source,
            dst_ref=place,
            send_sem=core_send.at[index],
            recv_sem=core_recv.at[index],
            device_id={"core": other},
            device_id_type=MESH,
        )

    started = []
    for position in range(len(orders[0])):
        for c, p in pieces:
            copy = hop(c, p, 0, orders[p][position])
            copy.start()
            started.append(copy)
    for c, p in pieces:
        copy = share(c, p, 0)
        copy.start()
        started.append(copy)
    load = pltpu.make_async_copy(x_ref, held, keep_sem.at[0])
    load.start()
    load.wait()
    store = pltpu.make_async_copy(held, out_ref.at[dp, core], keep_sem.at[1])
    store.start()
    for size in range(1, len(orders[0]) + 1):
        for c, p in pieces:
            order = orders[p]
            for mask in range(1, nd):
                if bin(mask).count("1") != size:
                    continue
                last = max(i for i, bit in enumerate(order) if mask & bit)
                hop(c, p, mask - order[last], order[last]).wait_recv()
                for bit in order[last + 1 :]:
                    copy = hop(c, p, mask, bit)
                    copy.start()
                    started.append(copy)
                copy = share(c, p, mask)
                copy.start()
                started.append(copy)
    for c, p in pieces:
        for mask in range(nd):
            share(c, p, mask).wait_recv()
    for copy in started:
        copy.wait_send()
    store.wait()


def collect_kernel(
    nd, order_out, x_ref, out_ref, mine, from_core, out_box, in_box, load_sem, send, recv, core_send, core_recv
):
    dp, core = lax.axis_index("dp"), lax.axis_index("core")
    other = 1 - core
    rows = out_ref.shape[0] // (PARTS * CHUNKS)
    greet(nd, dp, other)
    orders = hops(nd)

    def span(c, p):
        return pl.ds((p * CHUNKS + c) * rows, rows)

    def share(c, p, mask):
        index = (p * CHUNKS + c) * nd + mask
        return pltpu.make_async_remote_copy(
            src_ref=x_ref.at[flip(dp, mask), other, span(c, p)],
            dst_ref=from_core.at[mask, span(c, p)],
            send_sem=core_send.at[index],
            recv_sem=core_recv.at[index],
            device_id={"core": other},
            device_id_type=MESH,
        )

    def hop(c, p, mask):
        index = (p * CHUNKS + c) * nd + mask
        bit = next(bit for bit in orders[p] if mask & bit)
        return pltpu.make_async_remote_copy(
            src_ref=out_box.at[mask, span(c, p)],
            dst_ref=in_box.at[mask, span(c, p)],
            send_sem=send.at[index],
            recv_sem=recv.at[index],
            device_id={"dp": flip(dp, bit)},
            device_id_type=MESH,
        )

    def stage(p, mask):
        order = orders[p]
        return next((i for i, bit in enumerate(order) if mask & bit), len(order))

    steps = []
    for position in range(len(orders[0]) + 1):
        for c in range(CHUNKS):
            for p in range(PARTS):
                masks = [m for m in range(nd - 1, -1, -1) if stage(p, m) == position]
                steps += [(c, p, m) for m in masks]
    started = []
    for c, p, mask in steps:
        copy = share(c, p, mask)
        copy.start()
        started.append(copy)
    loads = [
        pltpu.make_async_copy(x_ref.at[flip(dp, mask), core], mine.at[mask], load_sem.at[mask])
        for mask in range(nd)
    ]
    for load in loads:
        load.start()
    for load in loads:
        load.wait()
    step_rows = 16
    for c, p, mask in steps:
        order = orders[p]
        arrived = [mask + bit for bit in order[: stage(p, mask)]]
        share(c, p, mask).wait_recv()
        for m in arrived:
            hop(c, p, m).wait_recv()
        first = (p * CHUNKS + c) * rows

        def add(i, carry, mask=mask, arrived=arrived, first=first):
            at = pl.ds(pl.multiple_of(first + i * step_rows, step_rows), step_rows)
            total = mine[mask, at].astype(f32) + from_core[mask, at].astype(f32)
            for m in arrived:
                total = total + in_box[m, at].astype(f32)
            if mask == 0:
                block = total.shape[1] // len(order_out)
                for place, source in enumerate(order_out):
                    out_ref[at, place * block : (place + 1) * block] = total[
                        :, source * block : (source + 1) * block
                    ]
            else:
                out_box[mask, at] = total.astype(bf16)
            return carry

        lax.fori_loop(0, rows // step_rows, add, 0)
        if mask:
            copy = hop(c, p, mask)
            copy.start()
            started.append(copy)
    for copy in started:
        copy.wait_send()


def place_kernel(nd, nz, nc, unit, parts_ref, out_ref):
    for d in range(nd):
        for c in range(nc):
            part = parts_ref[d * nc + c].astype(f32)
            for z in range(nz):
                at = ((d * nz + z) * nc + c) * unit
                out_ref[:, at : at + unit] = part[:, z * unit : (z + 1) * unit]


def place_columns(parts, nd, nz, nc, unit):
    held = parts.shape[1]
    return pl.pallas_call(
        functools.partial(place_kernel, nd, nz, nc, unit),
        out_shape=jax.ShapeDtypeStruct((held, nd * nz * nc * unit), f32),
        in_specs=[pl.BlockSpec(memory_space=pltpu.VMEM)],
        out_specs=pl.BlockSpec(memory_space=pltpu.VMEM),
        cost_estimate=pl.CostEstimate(
            flops=0, bytes_accessed=6 * parts.size, transcendentals=0
        ),
    )(parts)


def plane_gather(values, nd, nc, ident):
    rows, width = values.shape
    sems = PARTS * CHUNKS * nd
    out = pl.pallas_call(
        functools.partial(spread_kernel, nd),
        out_shape=jax.ShapeDtypeStruct((nd, nc, rows, width), values.dtype),
        in_specs=[pl.BlockSpec(memory_space=pl.ANY)],
        out_specs=pl.BlockSpec(memory_space=pl.ANY),
        scratch_shapes=[
            pltpu.VMEM((rows, width), values.dtype),
            pltpu.SemaphoreType.DMA((2,)),
            pltpu.SemaphoreType.DMA((sems,)),
            pltpu.SemaphoreType.DMA((sems,)),
            pltpu.SemaphoreType.DMA((sems,)),
            pltpu.SemaphoreType.DMA((sems,)),
        ],
        compiler_params=pltpu.CompilerParams(collective_id=ident, has_side_effects=True),
        cost_estimate=pl.CostEstimate(
            flops=0, bytes_accessed=16 * nd * rows * width, transcendentals=0
        ),
    )(values)
    return out.reshape(nd * nc * rows, width)


def plane_reduce(values, nd, nc, ident, order=(0,)):
    width = values.shape[1]
    rows = values.shape[0] // (nd * nc)
    sems = PARTS * CHUNKS * nd
    box = pltpu.VMEM((nd, rows, width), bf16)
    return pl.pallas_call(
        functools.partial(collect_kernel, nd, tuple(order)),
        out_shape=jax.ShapeDtypeStruct((rows, width), f32),
        in_specs=[pl.BlockSpec(memory_space=pl.ANY)],
        out_specs=pl.BlockSpec(memory_space=pltpu.VMEM),
        scratch_shapes=[
            box,
            box,
            box,
            box,
            pltpu.SemaphoreType.DMA((nd,)),
            pltpu.SemaphoreType.DMA((sems,)),
            pltpu.SemaphoreType.DMA((sems,)),
            pltpu.SemaphoreType.DMA((sems,)),
            pltpu.SemaphoreType.DMA((sems,)),
        ],
        compiler_params=pltpu.CompilerParams(collective_id=ident, has_side_effects=True),
        cost_estimate=pl.CostEstimate(
            flops=0, bytes_accessed=16 * nd * rows * width, transcendentals=0
        ),
    )(values.reshape(nd, nc, rows, width))


def local(
    tokens,
    cotangent,
    w_query,
    w_key,
    w_value,
    w_output,
    gain_attn,
    w_gate,
    w_up,
    w_down,
    gain_mlp,
    span_start,
    span_len,
):
    nd, nz, nc = lax.axis_size("dp"), lax.axis_size("zz"), lax.axis_size("core")
    plane = nd * nc
    seq_count, row_count, width = tokens.shape
    own = seq_count * row_count
    group = plane * own
    held = w_query.shape[0]
    ff_held = w_down.shape[0]
    heads = H // plane
    q_width = heads * HD
    seqs = nd * seq_count
    pics = span_start.shape[1]
    queries = nc * row_count
    zz, core = lax.axis_index("zz"), lax.axis_index("core")
    whole_heads = held % HD == 0

    def gather(values, ident):
        return plane_gather(values, nd, nc, ident)

    def reduce(values, ident):
        return plane_reduce(values, nd, nc, ident)

    feature_block = nc * held

    def to_weight_order(values):
        values = values.reshape(own, nd, nz, feature_block)
        return values.swapaxes(1, 2).reshape(own, width)

    def to_feature_order(values):
        values = values.reshape(own, nz, nd, feature_block)
        return values.swapaxes(1, 2).reshape(own, width)

    def reduce_features(values, ident):
        if feature_block % 128:
            return to_feature_order(reduce(values, ident))
        order = [z * nd + d for d in range(nd) for z in range(nz)]
        return plane_reduce(values, nd, nc, ident, order)

    tie = lax.optimization_barrier

    def by_member(weight, unit):
        weight = weight.reshape(held, nd, nz, nc, unit)
        return weight.transpose(1, 3, 0, 2, 4).reshape(plane, held, nz * unit)

    def from_member(parts, unit):
        parts = parts.reshape(nd, nc, held, nz, unit)
        return parts.transpose(2, 0, 3, 1, 4).reshape(held, nd * nz * nc * unit)

    if whole_heads:
        query_cols = by_member(w_query, held)
    else:
        query_cols = w_query.reshape(held, plane, q_width).transpose(1, 0, 2)
    share = plane // KVH
    key_cols = jnp.repeat(w_key.reshape(held, KVH, HD).transpose(1, 0, 2), share, axis=0)
    value_cols = jnp.repeat(w_value.reshape(held, KVH, HD).transpose(1, 0, 2), share, axis=0)
    qkv_width = q_width + 2 * HD
    ff_width = nz * ff_held

    def to_members(columns):
        return lax.all_to_all(columns, PLANE, 0, 0, tiled=True)

    def z_gather(values):
        return lax.all_gather(values, "zz", axis=0, tiled=True)

    spans = jnp.concatenate([span_start.reshape(-1), span_len.reshape(-1)])
    small = jnp.concatenate(
        [gain_attn, gain_mlp, (spans // 32).astype(bf16), (spans % 32).astype(bf16)]
    )
    small = jnp.pad(small, (0, qkv_width - small.shape[0]))
    small = jnp.broadcast_to(small, (plane, 1, qkv_width))
    small = jnp.pad(small, ((0, 0), (0, 15), (0, 0)))
    columns = jnp.concatenate(
        [jnp.concatenate([query_cols, key_cols, value_cols], axis=-1), small], axis=1
    )
    columns = z_gather(to_members(columns)).reshape(nz, nd, nc, held + 16, qkv_width)
    wqkv = columns[:, :, :, :held].reshape(width, qkv_width)
    small = columns[:, :, :, held]
    gains = small[..., : 2 * held].astype(f32)
    gain_a_weight_order = gains[..., :held].reshape(width)
    gains = gains.transpose(1, 0, 2, 3)
    gain_a = gains[..., :held].reshape(width)
    gain_m = gains[..., held:].reshape(width)
    split = seq_count * pics
    spans = small[0, :, 0, 2 * held : 2 * held + 4 * split].astype(jnp.int32)
    spans = spans[:, : 2 * split] * 32 + spans[:, 2 * split :]
    scalars = jnp.concatenate(
        [
            spans[:, :split].reshape(-1),
            spans[:, split:].reshape(-1),
            (zz * queries).astype(jnp.int32)[None],
        ]
    )

    if whole_heads:
        wo = z_gather(w_output)
    else:
        wo = lax.all_gather(w_output, ("zz", "core"), axis=0, tiled=True)
        wo = lax.dynamic_slice_in_dim(wo, core * q_width, q_width, 0)
    ff_columns = to_members(
        jnp.concatenate([by_member(w_gate, ff_held), by_member(w_up, ff_held)], axis=-1)
    )

    positions = (zz * queries + jnp.arange(queries, dtype=jnp.int32)).astype(f32)
    frequency = rope_base ** (-jnp.arange(HALF, dtype=f32) / HALF)
    angles = positions[:, None] * frequency[None, :]
    cosine, sine = jnp.cos(angles), jnp.sin(angles)
    cos_wide = jnp.tile(cosine, (1, q_width // HALF))
    sin_wide = jnp.tile(sine, (1, q_width // HALF))
    cos_k = cosine.reshape(1, nc, 1, row_count, HALF)
    sin_k = sine.reshape(1, nc, 1, row_count, HALF)

    x_low = tokens.reshape(own, width)
    x = x_low.astype(f32)
    inverse_attn = rms_scale(x)
    x_group = gather(to_weight_order(x_low), 1).astype(f32)
    normed = (x_group * rms_scale(x_group) * gain_a_weight_order).astype(bf16)
    dy_low = cotangent.reshape(own, width)

    pre = jnp.dot(normed, wqkv, preferred_element_type=f32)
    pre = pre.reshape(nd, nc, seq_count, row_count, qkv_width)
    ka, kb = pre[..., q_width : q_width + HALF], pre[..., q_width + HALF : q_width + HD]
    kv = jnp.concatenate(
        [ka * cos_k - kb * sin_k, kb * cos_k + ka * sin_k, pre[..., q_width + HD :]], axis=-1
    ).astype(bf16)
    kv = kv.transpose(0, 2, 1, 3, 4).reshape(seqs, queries, 2 * HD)
    kv, wo, dy_late = tie((kv, wo, dy_low))
    kv_all = lax.all_gather(kv, "zz", axis=1, tiled=True)
    dy_group = gather(dy_late, 2)
    kv_all, dy_group, ff_columns, down_rows = tie((kv_all, dy_group, ff_columns, w_down))
    wg = z_gather(ff_columns[:, :, :ff_width].reshape(plane * held, ff_width))
    wu = z_gather(ff_columns[:, :, ff_width:].reshape(plane * held, ff_width))
    wd = z_gather(down_rows)
    keys = nz * queries

    def token_block(columns_held):
        return pl.BlockSpec(
            (1, nc, 1, row_count, columns_held),
            lambda g, s: (g // seq_count, 0, lax.rem(g, seq_count), 0, 0),
        )

    table_block = pl.BlockSpec((queries, q_width), lambda g, s: (0, 0))
    kv_block = pl.BlockSpec((1, keys, 2 * HD), lambda g, s: (g, 0, 0))
    lse_block = pl.BlockSpec((1, heads, queries), lambda g, s: (g, 0, 0))
    token_shape = jax.ShapeDtypeStruct((nd, nc, seq_count, row_count, q_width), bf16)

    attended, q_kept, lse = pl.pallas_call(
        functools.partial(attend_kernel, pics, seqs, heads),
        out_shape=(
            token_shape,
            token_shape,
            jax.ShapeDtypeStruct((seqs, heads, queries), f32),
        ),
        grid_spec=pltpu.PrefetchScalarGridSpec(
            num_scalar_prefetch=1,
            grid=(seqs,),
            in_specs=[token_block(qkv_width), table_block, table_block, kv_block],
            out_specs=(token_block(q_width), token_block(q_width), lse_block),
        ),
        cost_estimate=pl.CostEstimate(
            flops=4 * seqs * heads * queries * keys * HD,
            bytes_accessed=8 * group * q_width,
            transcendentals=seqs * heads * queries * keys,
        ),
    )(scalars, pre, cos_wide, sin_wide, kv_all)

    attended = attended.reshape(group, q_width)
    mixed = reduce(jnp.dot(attended, wo, preferred_element_type=f32).astype(bf16), 5)
    middle = x + mixed
    inverse_mlp = rms_scale(middle)
    normed_mid = gather(
        to_weight_order((middle * inverse_mlp * gain_m).astype(bf16)), 3
    )
    gate = jnp.dot(normed_mid, wg, preferred_element_type=f32)
    up = jnp.dot(normed_mid, wu, preferred_element_type=f32)
    sigmoid = jax.nn.sigmoid(gate)
    hidden = (gate * sigmoid * up).astype(bf16)

    def columns_dot(left, right):
        return lax.dot_general(
            left, right, (((0,), (0,)), ((), ())), preferred_element_type=f32
        ).astype(bf16)

    def z_reduce(values):
        return lax.psum_scatter(values, "zz", scatter_dimension=0, tiled=True)

    def home(values):
        values = values.reshape(plane, held, values.shape[-1])
        return lax.all_to_all(values, PLANE, 0, 0, tiled=True)

    dy_late, weight_down = tie((dy_group, columns_dot(hidden, dy_group)))
    weight_down = z_reduce(weight_down).astype(f32)
    grad_hidden = rows_dot(dy_late, wd).astype(bf16).astype(f32)
    grad_gate = (grad_hidden * up * sigmoid * (1.0 + gate * (1.0 - sigmoid))).astype(bf16)
    grad_up = (grad_hidden * gate * sigmoid).astype(bf16)
    weight_gate = columns_dot(normed_mid, grad_gate)
    weight_up = columns_dot(normed_mid, grad_up)
    back_mid = (rows_dot(grad_gate, wg) + rows_dot(grad_up, wu)).astype(bf16)
    back_mid, weight_gate, weight_up = tie((back_mid, weight_gate, weight_up))
    weight_gate = z_reduce(weight_gate)
    weight_up = z_reduce(weight_up)
    weight_gate = place_columns(home(weight_gate), nd, nz, nc, ff_held)
    weight_up = place_columns(home(weight_up), nd, nz, nc, ff_held)

    grad_normed_mid = reduce_features(back_mid, 6)
    grad_middle_norm = rms_back(grad_normed_mid, middle, inverse_mlp, gain_m)
    grad_middle = dy_low.astype(f32) + grad_middle_norm
    mid_group = gather(grad_middle.astype(bf16), 4)
    grad_mix = rows_dot(mid_group, wo).astype(bf16)

    dq, dkv = pl.pallas_call(
        functools.partial(attend_back_kernel, pics, seqs, heads),
        out_shape=(token_shape, jax.ShapeDtypeStruct((seqs, keys, 2 * HD), bf16)),
        grid_spec=pltpu.PrefetchScalarGridSpec(
            num_scalar_prefetch=1,
            grid=(seqs,),
            in_specs=[
                token_block(q_width),
                token_block(q_width),
                table_block,
                table_block,
                kv_block,
                lse_block,
            ],
            out_specs=(token_block(q_width), kv_block),
        ),
        cost_estimate=pl.CostEstimate(
            flops=10 * seqs * heads * queries * keys * HD,
            bytes_accessed=8 * group * q_width,
            transcendentals=seqs * heads * queries * keys,
        ),
    )(
        scalars,
        q_kept,
        grad_mix.reshape(token_shape.shape),
        cos_wide,
        sin_wide,
        kv_all,
        lse,
    )
    down = jnp.dot(hidden, wd, preferred_element_type=f32).astype(bf16)
    down, dq, dkv = tie((down, dq, dkv))
    dkv = lax.psum_scatter(dkv, "zz", scatter_dimension=1, tiled=True)
    down = reduce(down, 7)
    down, dkv, attended_late = tie((down, dkv, attended))
    layer_out = (middle + down).astype(bf16).reshape(tokens.shape)
    dkv = dkv.astype(f32)
    dkv = dkv.reshape(nd, seq_count, nc, row_count, 2 * HD).transpose(0, 2, 1, 3, 4)
    da, db = dkv[..., :HALF], dkv[..., HALF:HD]
    dkv = jnp.concatenate(
        [da * cos_k + db * sin_k, db * cos_k - da * sin_k, dkv[..., HD:]], axis=-1
    ).astype(bf16)
    dqkv = jnp.concatenate(
        [dq.reshape(group, q_width), dkv.reshape(group, 2 * HD)], axis=-1
    )
    weight_qkv = columns_dot(normed, dqkv)
    back_in, weight_qkv = tie((rows_dot(dqkv, wqkv).astype(bf16), weight_qkv))
    weight_qkv = z_reduce(weight_qkv)
    weight_qkv = home(weight_qkv).astype(f32)
    weight_output = columns_dot(attended_late, mid_group)
    if whole_heads:
        weight_output = z_reduce(weight_output).astype(f32)
    else:
        spread = lax.dynamic_update_slice_in_dim(
            jnp.zeros((nc * q_width, width), bf16), weight_output, core * q_width, 0
        )
        weight_output = lax.psum_scatter(
            spread, ("zz", "core"), scatter_dimension=0, tiled=True
        ).astype(f32)
    grad_normed = reduce_features(back_in, 8)
    grad_input_norm = rms_back(grad_normed, x, inverse_attn, gain_a)
    input_grad = (grad_middle + grad_input_norm).astype(bf16).reshape(tokens.shape)

    if whole_heads:
        weight_query = from_member(weight_qkv[:, :, :q_width], held)
    else:
        weight_query = weight_qkv[:, :, :q_width].transpose(1, 0, 2).reshape(held, H * HD)

    def kv_home(parts):
        parts = jnp.sum(parts.reshape(KVH, share, held, HD), axis=1)
        return parts.transpose(1, 0, 2).reshape(held, KVH * HD)

    weight_key = kv_home(weight_qkv[:, :, q_width : q_width + HD])
    weight_value = kv_home(weight_qkv[:, :, q_width + HD :])

    def gain_grad(pairs, gain):
        terms = (jnp.sum(w.astype(f32) * grad, axis=1) for w, grad in pairs)
        return sum(terms) / gain.astype(f32)

    grad_gain_attn = gain_grad(
        ((w_query, weight_query), (w_key, weight_key), (w_value, weight_value)), gain_attn
    )
    grad_gain_mlp = gain_grad(((w_gate, weight_gate), (w_up, weight_up)), gain_mlp)
    return (
        layer_out,
        input_grad,
        weight_query,
        weight_key,
        weight_value,
        weight_output,
        grad_gain_attn,
        weight_gate,
        weight_up,
        weight_down,
        grad_gain_mlp,
    )


def solution(mesh):
    nd, ns = mesh.shape["dp"], mesh.shape["seq"]
    inner = Mesh(mesh.devices.reshape(nd, ns // 2, 2), ALL)
    rows = P("dp", ("zz", "core"), None)
    weight = P(ALL, None)
    gain = P(ALL)
    spans = P("dp", None)
    return jax.shard_map(
        local,
        mesh=inner,
        in_specs=(rows, rows) + (weight,) * 4 + (gain,) + (weight,) * 3 + (gain, spans, spans),
        out_specs=(rows, rows) + (weight,) * 4 + (gain,) + (weight,) * 3 + (gain,),
        check_vma=False,
    )
```

```python
import functools

import jax
import jax.numpy as jnp
from jax import lax
from jax.experimental import pallas as pl
from jax.experimental.pallas import tpu as pltpu
from jax.sharding import Mesh, PartitionSpec as P


H = 32
KVH = 4
HD = 64
HALF = HD // 2

epsilon = 1e-05
masked_value = -1e30
rope_base = 10000.0

PLANE = ("dp", "core")
ALL = ("dp", "zz", "core")
f32 = jnp.float32
bf16 = jnp.bfloat16


def rms_scale(values):
    return lax.rsqrt(jnp.mean(values * values, axis=-1, keepdims=True) + epsilon)


def rms_back(grad_normed, values, inverse, gain):
    scaled_grad = grad_normed * gain
    unit_rows = values * inverse
    grad_values = inverse * (
        scaled_grad - unit_rows * jnp.mean(scaled_grad * unit_rows, axis=-1, keepdims=True)
    )
    return grad_values


def swap_halves(values):
    width = values.shape[-1]
    lane = lax.broadcasted_iota(jnp.int32, values.shape, 1)
    ahead = pltpu.roll(values, width - HALF, 1)
    behind = pltpu.roll(values, HALF, 1)
    return jnp.where(lane % HD < HALF, -ahead, behind)


def span_bias(scalars, seq_index, pics, seqs, keys, queries):
    key_pos = lax.broadcasted_iota(jnp.int32, (keys, 1), 0)
    query_pos = lax.broadcasted_iota(jnp.int32, (1, queries), 1) + scalars[2 * seqs * pics]
    allowed = key_pos <= query_pos
    for k in range(pics):
        start = scalars[seq_index * pics + k]
        stop = start + scalars[seqs * pics + seq_index * pics + k]
        key_in = (key_pos >= start) & (key_pos < stop)
        query_in = (query_pos >= start) & (query_pos < stop)
        allowed = allowed | (key_in & query_in)
    return jnp.where(allowed, 0.0, masked_value).astype(f32)


def rows_dot(left, right):
    return lax.dot_general(left, right, (((1,), (1,)), ((), ())), preferred_element_type=f32)


def attend_kernel(pics, seqs, heads, scalars, pre_ref, cos_ref, sin_ref, kv_ref, out_ref, q_ref, lse_ref):
    seq_index = pl.program_id(0)
    cores, rows = pre_ref.shape[1], pre_ref.shape[3]
    queries, keys = cores * rows, kv_ref.shape[1]
    width = heads * HD
    pre = pre_ref[0, :, 0, :, :width].reshape(queries, width)
    q = (pre * cos_ref[...] + swap_halves(pre) * sin_ref[...]).astype(bf16) * bf16(0.125)
    q_ref[...] = q.reshape(q_ref.shape)
    kv = kv_ref[0]
    k = kv[:, :HD]
    v_t = kv.T[HD:]
    bias = span_bias(scalars, seq_index, pics, seqs, keys, queries)
    outs = []
    for h in range(heads):
        s = rows_dot(k, q[:, h * HD : (h + 1) * HD]) + bias
        top = jnp.max(s, axis=0, keepdims=True)
        e = jnp.exp(s - top)
        total = jnp.sum(e, axis=0, keepdims=True)
        p = (e * (1.0 / total)).astype(bf16)
        lse_ref[0, h : h + 1, :] = top + jnp.log(total)
        outs.append(jnp.dot(v_t, p, preferred_element_type=f32))
    out = jnp.concatenate(outs, axis=0).T.astype(bf16)
    out_ref[...] = out.reshape(out_ref.shape)


def attend_back_kernel(
    pics, seqs, heads, scalars, q_ref, do_ref, cos_ref, sin_ref, kv_ref, lse_ref, dq_ref, dkv_ref
):
    seq_index = pl.program_id(0)
    cores, rows = q_ref.shape[1], q_ref.shape[3]
    queries, keys = cores * rows, kv_ref.shape[1]
    width = heads * HD
    q = q_ref[...].reshape(queries, width)
    do = do_ref[...].reshape(queries, width)
    kv = kv_ref[0]
    k, v = kv[:, :HD], kv[:, HD:]
    k_t = kv.T[:HD]
    bias = span_bias(scalars, seq_index, pics, seqs, keys, queries)
    dk = jnp.zeros((keys, HD), f32)
    dv = jnp.zeros((keys, HD), f32)
    dqs = []
    for h in range(heads):
        q_h = q[:, h * HD : (h + 1) * HD]
        do_h = do[:, h * HD : (h + 1) * HD]
        p = jnp.exp(rows_dot(k, q_h) + bias - lse_ref[0, h : h + 1, :])
        dp = rows_dot(v, do_h)
        delta = jnp.sum(p * dp, axis=0, keepdims=True)
        ds = (p * (dp - delta)).astype(bf16)
        dv = dv + jnp.dot(p.astype(bf16), do_h, preferred_element_type=f32)
        dk = dk + jnp.dot(ds, q_h, preferred_element_type=f32)
        dqs.append(jnp.dot(k_t, ds, preferred_element_type=f32))
    dq = jnp.concatenate(dqs, axis=0).T * 0.125
    dqp = dq * cos_ref[...] - swap_halves(dq) * sin_ref[...]
    dq_ref[...] = dqp.astype(bf16).reshape(dq_ref.shape)
    dkv_ref[0] = jnp.concatenate([dk, dv], axis=1).astype(bf16)


MESH = pl.DeviceIdType.MESH
PARTS = 2
CHUNKS = 2


def flip(index, mask):
    bit = 1
    while bit <= mask:
        if mask & bit:
            index = index + bit - 2 * bit * (index // bit % 2)
        bit *= 2
    return index


def hops(nd):
    bits = [1 << i for i in range(nd.bit_length() - 1)]
    return (bits, bits[::-1])


def greet(nd, dp, other):
    barrier = pltpu.get_barrier_semaphore()
    bits = hops(nd)[0]
    for bit in bits:
        pl.semaphore_signal(
            barrier, inc=1, device_id={"dp": flip(dp, bit)}, device_id_type=MESH
        )
    pl.semaphore_signal(barrier, inc=1, device_id={"core": other}, device_id_type=MESH)
    pl.semaphore_wait(barrier, len(bits) + 1)


def spread_kernel(nd, x_ref, out_ref, held, keep_sem, send, recv, core_send, core_recv):
    dp, core = lax.axis_index("dp"), lax.axis_index("core")
    other = 1 - core
    rows = x_ref.shape[0] // (PARTS * CHUNKS)
    greet(nd, dp, other)
    orders = hops(nd)
    pieces = [(c, p) for c in range(CHUNKS) for p in range(PARTS)]

    def span(c, p):
        return pl.ds((p * CHUNKS + c) * rows, rows)

    def hop(c, p, mask, bit):
        place = out_ref.at[flip(dp, mask), core, span(c, p)]
        source = x_ref.at[span(c, p)] if mask == 0 else place
        index = (p * CHUNKS + c) * nd + mask + bit
        return pltpu.make_async_remote_copy(
            src_ref=source,
            dst_ref=place,
            send_sem=send.at[index],
            recv_sem=recv.at[index],
            device_id={"dp": flip(dp, bit)},
            device_id_type=MESH,
        )

    def share(c, p, mask):
        place = out_ref.at[flip(dp, mask), core, span(c, p)]
        source = x_ref.at[span(c, p)] if mask == 0 else place
        index = (p * CHUNKS + c) * nd + mask
        return pltpu.make_async_remote_copy(
            src_ref=source,
            dst_ref=place,
            send_sem=core_send.at[index],
            recv_sem=core_recv.at[index],
            device_id={"core": other},
            device_id_type=MESH,
        )

    started = []
    for position in range(len(orders[0])):
        for c, p in pieces:
            copy = hop(c, p, 0, orders[p][position])
            copy.start()
            started.append(copy)
    for c, p in pieces:
        copy = share(c, p, 0)
        copy.start()
        started.append(copy)
    load = pltpu.make_async_copy(x_ref, held, keep_sem.at[0])
    load.start()
    load.wait()
    store = pltpu.make_async_copy(held, out_ref.at[dp, core], keep_sem.at[1])
    store.start()
    for size in range(1, len(orders[0]) + 1):
        for c, p in pieces:
            order = orders[p]
            for mask in range(1, nd):
                if bin(mask).count("1") != size:
                    continue
                last = max(i for i, bit in enumerate(order) if mask & bit)
                hop(c, p, mask - order[last], order[last]).wait_recv()
                for bit in order[last + 1 :]:
                    copy = hop(c, p, mask, bit)
                    copy.start()
                    started.append(copy)
                copy = share(c, p, mask)
                copy.start()
                started.append(copy)
    for c, p in pieces:
        for mask in range(nd):
            share(c, p, mask).wait_recv()
    for copy in started:
        copy.wait_send()
    store.wait()


def collect_kernel(
    nd, order_out, x_ref, out_ref, mine, from_core, out_box, in_box, load_sem, send, recv, core_send, core_recv
):
    dp, core = lax.axis_index("dp"), lax.axis_index("core")
    other = 1 - core
    rows = out_ref.shape[0] // (PARTS * CHUNKS)
    greet(nd, dp, other)
    orders = hops(nd)

    def span(c, p):
        return pl.ds((p * CHUNKS + c) * rows, rows)

    def share(c, p, mask):
        index = (p * CHUNKS + c) * nd + mask
        return pltpu.make_async_remote_copy(
            src_ref=x_ref.at[flip(dp, mask), other, span(c, p)],
            dst_ref=from_core.at[mask, span(c, p)],
            send_sem=core_send.at[index],
            recv_sem=core_recv.at[index],
            device_id={"core": other},
            device_id_type=MESH,
        )

    def hop(c, p, mask):
        index = (p * CHUNKS + c) * nd + mask
        bit = next(bit for bit in orders[p] if mask & bit)
        return pltpu.make_async_remote_copy(
            src_ref=out_box.at[mask, span(c, p)],
            dst_ref=in_box.at[mask, span(c, p)],
            send_sem=send.at[index],
            recv_sem=recv.at[index],
            device_id={"dp": flip(dp, bit)},
            device_id_type=MESH,
        )

    def stage(p, mask):
        order = orders[p]
        return next((i for i, bit in enumerate(order) if mask & bit), len(order))

    steps = []
    for position in range(len(orders[0]) + 1):
        for c in range(CHUNKS):
            for p in range(PARTS):
                masks = [m for m in range(nd - 1, -1, -1) if stage(p, m) == position]
                steps += [(c, p, m) for m in masks]
    started = []
    for c, p, mask in steps:
        copy = share(c, p, mask)
        copy.start()
        started.append(copy)
    loads = [
        pltpu.make_async_copy(x_ref.at[flip(dp, mask), core], mine.at[mask], load_sem.at[mask])
        for mask in range(nd)
    ]
    for load in loads:
        load.start()
    for load in loads:
        load.wait()
    step_rows = 16
    for c, p, mask in steps:
        order = orders[p]
        arrived = [mask + bit for bit in order[: stage(p, mask)]]
        share(c, p, mask).wait_recv()
        for m in arrived:
            hop(c, p, m).wait_recv()
        first = (p * CHUNKS + c) * rows

        def add(i, carry, mask=mask, arrived=arrived, first=first):
            at = pl.ds(pl.multiple_of(first + i * step_rows, step_rows), step_rows)
            total = mine[mask, at].astype(f32) + from_core[mask, at].astype(f32)
            for m in arrived:
                total = total + in_box[m, at].astype(f32)
            if mask == 0:
                block = total.shape[1] // len(order_out)
                for place, source in enumerate(order_out):
                    out_ref[at, place * block : (place + 1) * block] = total[
                        :, source * block : (source + 1) * block
                    ]
            else:
                out_box[mask, at] = total.astype(bf16)
            return carry

        lax.fori_loop(0, rows // step_rows, add, 0)
        if mask:
            copy = hop(c, p, mask)
            copy.start()
            started.append(copy)
    for copy in started:
        copy.wait_send()


def blocks_of(values, order):
    block = values.shape[1] // len(order)
    return jnp.concatenate(
        [values[:, source * block : (source + 1) * block] for source in order], axis=1
    )


def pivot_kernel(
    nd,
    forward,
    orders_out,
    part_ref,
    own_ref,
    gain_ref,
    *rest,
):
    middle_ref = None
    if not forward:
        middle_ref, rest = rest[0], rest[1:]
    (
        row_ref,
        group_ref,
        mine,
        from_core,
        out_box,
        in_box,
        held,
        load_sem,
        send,
        recv,
        core_send,
        core_recv,
        keep_sem,
        send2,
        recv2,
        core_send2,
        core_recv2,
    ) = rest
    dp, core = lax.axis_index("dp"), lax.axis_index("core")
    other = 1 - core
    rows = row_ref.shape[0] // (PARTS * CHUNKS)
    greet(nd, dp, other)
    orders = hops(nd)
    pieces = [(c, p) for c in range(CHUNKS) for p in range(PARTS)]

    def span(c, p):
        return pl.ds((p * CHUNKS + c) * rows, rows)

    def slot(c, p, mask):
        return (p * CHUNKS + c) * nd + mask

    def share(c, p, mask):
        index = slot(c, p, mask)
        return pltpu.make_async_remote_copy(
            src_ref=part_ref.at[flip(dp, mask), other, span(c, p)],
            dst_ref=from_core.at[mask, span(c, p)],
            send_sem=core_send.at[index],
            recv_sem=core_recv.at[index],
            device_id={"core": other},
            device_id_type=MESH,
        )

    def hop(c, p, mask):
        index = slot(c, p, mask)
        bit = next(bit for bit in orders[p] if mask & bit)
        return pltpu.make_async_remote_copy(
            src_ref=out_box.at[mask, span(c, p)],
            dst_ref=in_box.at[mask, span(c, p)],
            send_sem=send.at[index],
            recv_sem=recv.at[index],
            device_id={"dp": flip(dp, bit)},
            device_id_type=MESH,
        )

    def hop_out(c, p, mask, bit):
        place = group_ref.at[flip(dp, mask), core, span(c, p)]
        index = slot(c, p, mask + bit)
        return pltpu.make_async_remote_copy(
            src_ref=held.at[span(c, p)] if mask == 0 else place,
            dst_ref=place,
            send_sem=send2.at[index],
            recv_sem=recv2.at[index],
            device_id={"dp": flip(dp, bit)},
            device_id_type=MESH,
        )

    def share_out(c, p, mask):
        place = group_ref.at[flip(dp, mask), core, span(c, p)]
        index = slot(c, p, mask)
        return pltpu.make_async_remote_copy(
            src_ref=held.at[span(c, p)] if mask == 0 else place,
            dst_ref=place,
            send_sem=core_send2.at[index],
            recv_sem=core_recv2.at[index],
            device_id={"core": other},
            device_id_type=MESH,
        )

    def stage(p, mask):
        order = orders[p]
        return next((i for i, bit in enumerate(order) if mask & bit), len(order))

    steps = []
    for position in range(len(orders[0]) + 1):
        for c, p in pieces:
            masks = [m for m in range(nd - 1, -1, -1) if stage(p, m) == position]
            steps += [(c, p, m) for m in masks]
    started = []
    for c, p, mask in steps:
        copy = share(c, p, mask)
        copy.start()
        started.append(copy)
    loads = [
        pltpu.make_async_copy(part_ref.at[flip(dp, mask), core], mine.at[mask], load_sem.at[mask])
        for mask in range(nd)
    ]
    for load in loads:
        load.start()
    for load in loads:
        load.wait()
    step_rows = 16
    gain = gain_ref[...]
    kept = []

    def finish(total, at):
        if forward:
            middle = own_ref[at].astype(f32) + total
            inverse = rms_scale(middle)
            row_ref[at] = middle
            held[at] = blocks_of((middle * inverse * gain).astype(bf16), orders_out)
            return
        middle = middle_ref[at]
        inverse = rms_scale(middle)
        grad = own_ref[at].astype(f32) + rms_back(
            blocks_of(total, orders_out), middle, inverse, gain
        )
        row_ref[at] = grad
        held[at] = grad.astype(bf16)

    for c, p, mask in steps:
        order = orders[p]
        arrived = [mask + bit for bit in order[: stage(p, mask)]]
        share(c, p, mask).wait_recv()
        for m in arrived:
            hop(c, p, m).wait_recv()
        first = (p * CHUNKS + c) * rows

        def add(i, carry, mask=mask, arrived=arrived, first=first):
            at = pl.ds(pl.multiple_of(first + i * step_rows, step_rows), step_rows)
            total = mine[mask, at].astype(f32) + from_core[mask, at].astype(f32)
            for m in arrived:
                total = total + in_box[m, at].astype(f32)
            if mask == 0:
                finish(total, at)
            else:
                out_box[mask, at] = total.astype(bf16)
            return carry

        lax.fori_loop(0, rows // step_rows, add, 0)
        copies = [hop(c, p, mask)] if mask else []
        if mask == 0:
            copies = [hop_out(c, p, 0, bit) for bit in order] + [share_out(c, p, 0)]
            keep = pltpu.make_async_copy(
                held.at[span(c, p)],
                group_ref.at[dp, core, span(c, p)],
                keep_sem.at[p * CHUNKS + c],
            )
            keep.start()
            kept.append(keep)
        for copy in copies:
            copy.start()
            started.append(copy)
    for size in range(1, len(orders[0]) + 1):
        for c, p in pieces:
            order = orders[p]
            for mask in range(1, nd):
                if bin(mask).count("1") != size:
                    continue
                last = max(i for i, bit in enumerate(order) if mask & bit)
                hop_out(c, p, mask - order[last], order[last]).wait_recv()
                copies = [hop_out(c, p, mask, bit) for bit in order[last + 1 :]]
                for copy in copies + [share_out(c, p, mask)]:
                    copy.start()
                    started.append(copy)
    for c, p in pieces:
        for mask in range(nd):
            share_out(c, p, mask).wait_recv()
    for copy in started:
        copy.wait_send()
    for keep in kept:
        keep.wait()


def plane_pivot(part, own, gain, middle, nd, nc, ident, order):
    rows, width = own.shape
    sems = PARTS * CHUNKS * nd
    box = pltpu.VMEM((nd, rows, width), bf16)
    dma = pltpu.SemaphoreType.DMA
    whole = pl.BlockSpec(memory_space=pltpu.VMEM)
    extra = () if middle is None else (middle,)
    out, group = pl.pallas_call(
        functools.partial(pivot_kernel, nd, middle is None, tuple(order)),
        out_shape=(
            jax.ShapeDtypeStruct((rows, width), f32),
            jax.ShapeDtypeStruct((nd, nc, rows, width), bf16),
        ),
        in_specs=[pl.BlockSpec(memory_space=pl.ANY)] + [whole] * (2 + len(extra)),
        out_specs=(whole, pl.BlockSpec(memory_space=pl.ANY)),
        scratch_shapes=[box, box, box, box, pltpu.VMEM((rows, width), bf16), dma((nd,))]
        + [dma((sems,))] * 4
        + [dma((PARTS * CHUNKS,))]
        + [dma((sems,))] * 4,
        compiler_params=pltpu.CompilerParams(collective_id=ident, has_side_effects=True),
        cost_estimate=pl.CostEstimate(
            flops=0, bytes_accessed=32 * nd * rows * width, transcendentals=0
        ),
    )(part.reshape(nd, nc, rows, width), own, gain.reshape(1, width), *extra)
    return out, group.reshape(nd * nc * rows, width)


def split_kernel(nd, nz, nc, unit, gate_ref, up_ref, out_ref):
    for g, weight_ref in enumerate((gate_ref, up_ref)):
        weight = weight_ref[...].astype(f32)
        for d in range(nd):
            for c in range(nc):
                for z in range(nz):
                    at = ((d * nz + z) * nc + c) * unit
                    to = (g * nz + z) * unit
                    out_ref[d * nc + c, :, to : to + unit] = weight[:, at : at + unit].astype(bf16)


def split_columns(gate, up, nd, nz, nc, unit):
    held = gate.shape[0]
    whole = pl.BlockSpec(memory_space=pltpu.VMEM)
    return pl.pallas_call(
        functools.partial(split_kernel, nd, nz, nc, unit),
        out_shape=jax.ShapeDtypeStruct((nd * nc, held, 2 * nz * unit), bf16),
        in_specs=[whole, whole],
        out_specs=whole,
        cost_estimate=pl.CostEstimate(flops=0, bytes_accessed=8 * gate.size, transcendentals=0),
    )(gate, up)


def place_kernel(nd, nz, nc, unit, parts_ref, out_ref):
    for d in range(nd):
        for c in range(nc):
            part = parts_ref[d * nc + c].astype(f32)
            for z in range(nz):
                at = ((d * nz + z) * nc + c) * unit
                out_ref[:, at : at + unit] = part[:, z * unit : (z + 1) * unit]


def place_columns(parts, nd, nz, nc, unit):
    held = parts.shape[1]
    return pl.pallas_call(
        functools.partial(place_kernel, nd, nz, nc, unit),
        out_shape=jax.ShapeDtypeStruct((held, nd * nz * nc * unit), f32),
        in_specs=[pl.BlockSpec(memory_space=pltpu.VMEM)],
        out_specs=pl.BlockSpec(memory_space=pltpu.VMEM),
        cost_estimate=pl.CostEstimate(
            flops=0, bytes_accessed=6 * parts.size, transcendentals=0
        ),
    )(parts)


def plane_gather(values, nd, nc, ident):
    rows, width = values.shape
    sems = PARTS * CHUNKS * nd
    out = pl.pallas_call(
        functools.partial(spread_kernel, nd),
        out_shape=jax.ShapeDtypeStruct((nd, nc, rows, width), values.dtype),
        in_specs=[pl.BlockSpec(memory_space=pl.ANY)],
        out_specs=pl.BlockSpec(memory_space=pl.ANY),
        scratch_shapes=[
            pltpu.VMEM((rows, width), values.dtype),
            pltpu.SemaphoreType.DMA((2,)),
            pltpu.SemaphoreType.DMA((sems,)),
            pltpu.SemaphoreType.DMA((sems,)),
            pltpu.SemaphoreType.DMA((sems,)),
            pltpu.SemaphoreType.DMA((sems,)),
        ],
        compiler_params=pltpu.CompilerParams(collective_id=ident, has_side_effects=True),
        cost_estimate=pl.CostEstimate(
            flops=0, bytes_accessed=16 * nd * rows * width, transcendentals=0
        ),
    )(values)
    return out.reshape(nd * nc * rows, width)


def plane_reduce(values, nd, nc, ident, order=(0,)):
    width = values.shape[1]
    rows = values.shape[0] // (nd * nc)
    sems = PARTS * CHUNKS * nd
    box = pltpu.VMEM((nd, rows, width), bf16)
    return pl.pallas_call(
        functools.partial(collect_kernel, nd, tuple(order)),
        out_shape=jax.ShapeDtypeStruct((rows, width), f32),
        in_specs=[pl.BlockSpec(memory_space=pl.ANY)],
        out_specs=pl.BlockSpec(memory_space=pltpu.VMEM),
        scratch_shapes=[
            box,
            box,
            box,
            box,
            pltpu.SemaphoreType.DMA((nd,)),
            pltpu.SemaphoreType.DMA((sems,)),
            pltpu.SemaphoreType.DMA((sems,)),
            pltpu.SemaphoreType.DMA((sems,)),
            pltpu.SemaphoreType.DMA((sems,)),
        ],
        compiler_params=pltpu.CompilerParams(collective_id=ident, has_side_effects=True),
        cost_estimate=pl.CostEstimate(
            flops=0, bytes_accessed=16 * nd * rows * width, transcendentals=0
        ),
    )(values.reshape(nd, nc, rows, width))


def local(
    tokens,
    cotangent,
    w_query,
    w_key,
    w_value,
    w_output,
    gain_attn,
    w_gate,
    w_up,
    w_down,
    gain_mlp,
    span_start,
    span_len,
):
    nd, nz, nc = lax.axis_size("dp"), lax.axis_size("zz"), lax.axis_size("core")
    plane = nd * nc
    seq_count, row_count, width = tokens.shape
    own = seq_count * row_count
    group = plane * own
    held = w_query.shape[0]
    ff_held = w_down.shape[0]
    heads = H // plane
    q_width = heads * HD
    seqs = nd * seq_count
    pics = span_start.shape[1]
    queries = nc * row_count
    zz, core = lax.axis_index("zz"), lax.axis_index("core")
    whole_heads = held % HD == 0

    def gather(values, ident):
        return plane_gather(values, nd, nc, ident)

    def reduce(values, ident):
        return plane_reduce(values, nd, nc, ident)

    feature_block = nc * held

    def to_weight_order(values):
        values = values.reshape(own, nd, nz, feature_block)
        return values.swapaxes(1, 2).reshape(own, width)

    def to_feature_order(values):
        values = values.reshape(own, nz, nd, feature_block)
        return values.swapaxes(1, 2).reshape(own, width)

    def reduce_features(values, ident):
        if feature_block % 128:
            return to_feature_order(reduce(values, ident))
        order = [z * nd + d for d in range(nd) for z in range(nz)]
        return plane_reduce(values, nd, nc, ident, order)

    tie = lax.optimization_barrier

    def by_member(weight, unit):
        weight = weight.reshape(held, nd, nz, nc, unit)
        return weight.transpose(1, 3, 0, 2, 4).reshape(plane, held, nz * unit)

    def from_member(parts, unit):
        parts = parts.reshape(nd, nc, held, nz, unit)
        return parts.transpose(2, 0, 3, 1, 4).reshape(held, nd * nz * nc * unit)

    if whole_heads:
        query_cols = by_member(w_query, held)
    else:
        query_cols = w_query.reshape(held, plane, q_width).transpose(1, 0, 2)
    share = plane // KVH
    key_cols = jnp.repeat(w_key.reshape(held, KVH, HD).transpose(1, 0, 2), share, axis=0)
    value_cols = jnp.repeat(w_value.reshape(held, KVH, HD).transpose(1, 0, 2), share, axis=0)
    qkv_width = q_width + 2 * HD
    ff_width = nz * ff_held

    def to_members(columns):
        return lax.all_to_all(columns, PLANE, 0, 0, tiled=True)

    def z_gather(values):
        return lax.all_gather(values, "zz", axis=0, tiled=True)

    spans = jnp.concatenate([span_start.reshape(-1), span_len.reshape(-1)])
    small = jnp.concatenate(
        [gain_attn, gain_mlp, (spans // 32).astype(bf16), (spans % 32).astype(bf16)]
    )
    small = jnp.pad(small, (0, qkv_width - small.shape[0]))
    small = jnp.broadcast_to(small, (plane, 1, qkv_width))
    small = jnp.pad(small, ((0, 0), (0, 15), (0, 0)))
    columns = jnp.concatenate(
        [jnp.concatenate([query_cols, key_cols, value_cols], axis=-1), small], axis=1
    )
    columns = z_gather(to_members(columns)).reshape(nz, nd, nc, held + 16, qkv_width)
    wqkv = columns[:, :, :, :held].reshape(width, qkv_width)
    small = columns[:, :, :, held]
    gains = small[..., : 2 * held].astype(f32)
    gain_a_weight_order = gains[..., :held].reshape(width)
    gains = gains.transpose(1, 0, 2, 3)
    gain_a = gains[..., :held].reshape(width)
    gain_m = gains[..., held:].reshape(width)
    split = seq_count * pics
    spans = small[0, :, 0, 2 * held : 2 * held + 4 * split].astype(jnp.int32)
    spans = spans[:, : 2 * split] * 32 + spans[:, 2 * split :]
    scalars = jnp.concatenate(
        [
            spans[:, :split].reshape(-1),
            spans[:, split:].reshape(-1),
            (zz * queries).astype(jnp.int32)[None],
        ]
    )

    if whole_heads:
        wo = z_gather(w_output)
    else:
        wo = lax.all_gather(w_output, ("zz", "core"), axis=0, tiled=True)
        wo = lax.dynamic_slice_in_dim(wo, core * q_width, q_width, 0)
    ff_columns = to_members(split_columns(w_gate, w_up, nd, nz, nc, ff_held))

    positions = (zz * queries + jnp.arange(queries, dtype=jnp.int32)).astype(f32)
    frequency = rope_base ** (-jnp.arange(HALF, dtype=f32) / HALF)
    angles = positions[:, None] * frequency[None, :]
    cosine, sine = jnp.cos(angles), jnp.sin(angles)
    cos_wide = jnp.tile(cosine, (1, q_width // HALF))
    sin_wide = jnp.tile(sine, (1, q_width // HALF))
    cos_k = cosine.reshape(1, nc, 1, row_count, HALF)
    sin_k = sine.reshape(1, nc, 1, row_count, HALF)

    x_low = tokens.reshape(own, width)
    x = x_low.astype(f32)
    inverse_attn = rms_scale(x)
    x_group = gather(to_weight_order(x_low), 1).astype(f32)
    normed = (x_group * rms_scale(x_group) * gain_a_weight_order).astype(bf16)
    dy_low = cotangent.reshape(own, width)

    pre = jnp.dot(normed, wqkv, preferred_element_type=f32)
    pre = pre.reshape(nd, nc, seq_count, row_count, qkv_width)
    ka, kb = pre[..., q_width : q_width + HALF], pre[..., q_width + HALF : q_width + HD]
    kv = jnp.concatenate(
        [ka * cos_k - kb * sin_k, kb * cos_k + ka * sin_k, pre[..., q_width + HD :]], axis=-1
    ).astype(bf16)
    kv = kv.transpose(0, 2, 1, 3, 4).reshape(seqs, queries, 2 * HD)
    kv, wo, dy_late = tie((kv, wo, dy_low))
    kv_all = lax.all_gather(kv, "zz", axis=1, tiled=True)
    dy_group = gather(dy_late, 2)
    kv_all, dy_group, ff_columns, down_rows = tie((kv_all, dy_group, ff_columns, w_down))
    wg = z_gather(ff_columns[:, :, :ff_width].reshape(plane * held, ff_width))
    wu = z_gather(ff_columns[:, :, ff_width:].reshape(plane * held, ff_width))
    wd = z_gather(down_rows)
    keys = nz * queries

    def token_block(columns_held):
        return pl.BlockSpec(
            (1, nc, 1, row_count, columns_held),
            lambda g, s: (g // seq_count, 0, lax.rem(g, seq_count), 0, 0),
        )

    table_block = pl.BlockSpec((queries, q_width), lambda g, s: (0, 0))
    kv_block = pl.BlockSpec((1, keys, 2 * HD), lambda g, s: (g, 0, 0))
    lse_block = pl.BlockSpec((1, heads, queries), lambda g, s: (g, 0, 0))
    token_shape = jax.ShapeDtypeStruct((nd, nc, seq_count, row_count, q_width), bf16)

    attended, q_kept, lse = pl.pallas_call(
        functools.partial(attend_kernel, pics, seqs, heads),
        out_shape=(
            token_shape,
            token_shape,
            jax.ShapeDtypeStruct((seqs, heads, queries), f32),
        ),
        grid_spec=pltpu.PrefetchScalarGridSpec(
            num_scalar_prefetch=1,
            grid=(seqs,),
            in_specs=[token_block(qkv_width), table_block, table_block, kv_block],
            out_specs=(token_block(q_width), token_block(q_width), lse_block),
        ),
        cost_estimate=pl.CostEstimate(
            flops=4 * seqs * heads * queries * keys * HD,
            bytes_accessed=8 * group * q_width,
            transcendentals=seqs * heads * queries * keys,
        ),
    )(scalars, pre, cos_wide, sin_wide, kv_all)

    attended = attended.reshape(group, q_width)
    mixed = jnp.dot(attended, wo, preferred_element_type=f32).astype(bf16)
    if feature_block % 128:
        middle = x + reduce(mixed, 5)
        inverse_mlp = rms_scale(middle)
        normed_mid = gather(to_weight_order((middle * inverse_mlp * gain_m).astype(bf16)), 3)
    else:
        order = [d * nz + z for z in range(nz) for d in range(nd)]
        middle, normed_mid = plane_pivot(mixed, x_low, gain_m, None, nd, nc, 5, order)
    gate = jnp.dot(normed_mid, wg, preferred_element_type=f32)
    up = jnp.dot(normed_mid, wu, preferred_element_type=f32)
    sigmoid = jax.nn.sigmoid(gate)
    hidden = (gate * sigmoid * up).astype(bf16)

    def columns_dot(left, right):
        return lax.dot_general(
            left, right, (((0,), (0,)), ((), ())), preferred_element_type=f32
        ).astype(bf16)

    def z_reduce(values):
        return lax.psum_scatter(values, "zz", scatter_dimension=0, tiled=True)

    def home(values):
        values = values.reshape(plane, held, values.shape[-1])
        return lax.all_to_all(values, PLANE, 0, 0, tiled=True)

    dy_late, weight_down = tie((dy_group, columns_dot(hidden, dy_group)))
    weight_down = z_reduce(weight_down).astype(f32)
    grad_hidden = rows_dot(dy_late, wd).astype(bf16).astype(f32)
    grad_gate = (grad_hidden * up * sigmoid * (1.0 + gate * (1.0 - sigmoid))).astype(bf16)
    grad_up = (grad_hidden * gate * sigmoid).astype(bf16)
    weight_gate = columns_dot(normed_mid, grad_gate)
    weight_up = columns_dot(normed_mid, grad_up)
    back_mid = (rows_dot(grad_gate, wg) + rows_dot(grad_up, wu)).astype(bf16)
    weight_gate = z_reduce(weight_gate)
    weight_up = z_reduce(weight_up)
    weight_gate = place_columns(home(weight_gate), nd, nz, nc, ff_held)
    weight_up = place_columns(home(weight_up), nd, nz, nc, ff_held)

    if feature_block % 128:
        grad_middle = dy_low.astype(f32) + rms_back(
            reduce_features(back_mid, 6), middle, inverse_mlp, gain_m
        )
        mid_group = gather(grad_middle.astype(bf16), 4)
    else:
        order = [z * nd + d for d in range(nd) for z in range(nz)]
        grad_middle, mid_group = plane_pivot(back_mid, dy_low, gain_m, middle, nd, nc, 6, order)
    grad_mix = rows_dot(mid_group, wo).astype(bf16)

    dq, dkv = pl.pallas_call(
        functools.partial(attend_back_kernel, pics, seqs, heads),
        out_shape=(token_shape, jax.ShapeDtypeStruct((seqs, keys, 2 * HD), bf16)),
        grid_spec=pltpu.PrefetchScalarGridSpec(
            num_scalar_prefetch=1,
            grid=(seqs,),
            in_specs=[
                token_block(q_width),
                token_block(q_width),
                table_block,
                table_block,
                kv_block,
                lse_block,
            ],
            out_specs=(token_block(q_width), kv_block),
        ),
        cost_estimate=pl.CostEstimate(
            flops=10 * seqs * heads * queries * keys * HD,
            bytes_accessed=8 * group * q_width,
            transcendentals=seqs * heads * queries * keys,
        ),
    )(
        scalars,
        q_kept,
        grad_mix.reshape(token_shape.shape),
        cos_wide,
        sin_wide,
        kv_all,
        lse,
    )
    down = jnp.dot(hidden, wd, preferred_element_type=f32).astype(bf16)
    down, dq, dkv = tie((down, dq, dkv))
    dkv = lax.psum_scatter(dkv, "zz", scatter_dimension=1, tiled=True)
    down = reduce(down, 7)
    down, dkv, attended_late = tie((down, dkv, attended))
    layer_out = (middle + down).astype(bf16).reshape(tokens.shape)
    dkv = dkv.astype(f32)
    dkv = dkv.reshape(nd, seq_count, nc, row_count, 2 * HD).transpose(0, 2, 1, 3, 4)
    da, db = dkv[..., :HALF], dkv[..., HALF:HD]
    dkv = jnp.concatenate(
        [da * cos_k + db * sin_k, db * cos_k - da * sin_k, dkv[..., HD:]], axis=-1
    ).astype(bf16)
    dqkv = jnp.concatenate(
        [dq.reshape(group, q_width), dkv.reshape(group, 2 * HD)], axis=-1
    )
    weight_qkv = columns_dot(normed, dqkv)
    back_in, weight_qkv = tie((rows_dot(dqkv, wqkv).astype(bf16), weight_qkv))
    weight_qkv = z_reduce(weight_qkv)
    weight_qkv = home(weight_qkv).astype(f32)
    weight_output = columns_dot(attended_late, mid_group)
    if whole_heads:
        weight_output = z_reduce(weight_output).astype(f32)
    else:
        spread = lax.dynamic_update_slice_in_dim(
            jnp.zeros((nc * q_width, width), bf16), weight_output, core * q_width, 0
        )
        weight_output = lax.psum_scatter(
            spread, ("zz", "core"), scatter_dimension=0, tiled=True
        ).astype(f32)
    grad_normed = reduce_features(back_in, 8)
    grad_input_norm = rms_back(grad_normed, x, inverse_attn, gain_a)
    input_grad = (grad_middle + grad_input_norm).astype(bf16).reshape(tokens.shape)

    if whole_heads:
        weight_query = from_member(weight_qkv[:, :, :q_width], held)
    else:
        weight_query = weight_qkv[:, :, :q_width].transpose(1, 0, 2).reshape(held, H * HD)

    def kv_home(parts):
        parts = jnp.sum(parts.reshape(KVH, share, held, HD), axis=1)
        return parts.transpose(1, 0, 2).reshape(held, KVH * HD)

    weight_key = kv_home(weight_qkv[:, :, q_width : q_width + HD])
    weight_value = kv_home(weight_qkv[:, :, q_width + HD :])

    def gain_grad(pairs, gain):
        terms = (jnp.sum(w.astype(f32) * grad, axis=1) for w, grad in pairs)
        return sum(terms) / gain.astype(f32)

    grad_gain_attn = gain_grad(
        ((w_query, weight_query), (w_key, weight_key), (w_value, weight_value)), gain_attn
    )
    grad_gain_mlp = gain_grad(((w_gate, weight_gate), (w_up, weight_up)), gain_mlp)
    return (
        layer_out,
        input_grad,
        weight_query,
        weight_key,
        weight_value,
        weight_output,
        grad_gain_attn,
        weight_gate,
        weight_up,
        weight_down,
        grad_gain_mlp,
    )


def solution(mesh):
    nd, ns = mesh.shape["dp"], mesh.shape["seq"]
    inner = Mesh(mesh.devices.reshape(nd, ns // 2, 2), ALL)
    rows = P("dp", ("zz", "core"), None)
    weight = P(ALL, None)
    gain = P(ALL)
    spans = P("dp", None)
    return jax.shard_map(
        local,
        mesh=inner,
        in_specs=(rows, rows) + (weight,) * 4 + (gain,) + (weight,) * 3 + (gain, spans, spans),
        out_specs=(rows, rows) + (weight,) * 4 + (gain,) + (weight,) * 3 + (gain,),
        check_vma=False,
    )
```
